32 devices in a mesh: sample: 4 (over y, x), gz: 8 (over z, core).
Axes of the slice: x: 2, y: 2, z: 4, core: 2. Of those that a mesh axis runs over, the one named last changes fastest.
Arguments:
- field_now: float32 [12, 16, 160, 256], P('sample', 'gz'), parts along dimension 0, may hold values from -6 to 6
- field_before: float32 [12, 16, 160, 256], P('sample', 'gz'), parts along dimension 0, may hold values from -6 to 6
- lame_lambda: float32 [16, 640, 256], P('gz', 'sample'), parts along dimension 1, may hold values from 0.5 to 1.5
- shear_modulus: float32 [16, 640, 256], P('gz', 'sample'), parts along dimension 1, may hold values from 0.5 to 1.5
- density: float32 [16, 640, 256], P('gz', 'sample'), parts along dimension 1, may hold values from 1 to 2
- source_field: float32 [12, 16, 160, 256], P('sample', 'gz'), parts along dimension 0, may hold values from -6 to 6
- wavelet: float32 [32], P('sample'), parts along dimension 0, may hold values from -4 to 4
- prior_mean: float32 [16, 640, 256], P('gz', 'sample'), parts along dimension 1, may hold values from 0.5 to 1.5
- steps_taken: float32 [16, 16, 160, 256], P('sample', 'gz'), parts along dimension 0
- grad_change: float32 [16, 16, 160, 256], P('sample', 'gz'), parts along dimension 0, as said below
Outputs:
- field_final: float32 [12, 16, 160, 256], P('sample', 'gz'), parts along dimension 0
- gradient: float32 [16, 640, 256], P('gz', 'sample'), parts along dimension 1
- direction: float32 [16, 640, 256], P('gz', 'sample'), parts along dimension 1
The draws below stay inside these ranges and needn't reach their ends.
There are 4 independent parts, one for each index of `sample`. The reference program is written for one: setup_inputs(seed, part) draws one part's arguments, and reference() takes and returns one part's arrays. A program takes and returns all parts, laid end to end along the dimension named above; each array names one. Nothing has to cross between parts.
Inputs may be any that keep to these rules, and one draw needn't show every extreme that they name: Each entry of grad_change is 0.5 to 2 times the matching entry of steps_taken.
All inputs are finite; a program needn't handle non-finite values.
Results may differ from the reference program's by a relative error of at most 0.0003.
Values sent between devices are 32-bit elements; how exact they have to be, the bound alone decides.
A program may use at most 64 MiB of HBM per device.

```python
import math
import jax
import jax.numpy as jnp
from jax import lax

NX = 160
NY = 256
STEPS = 8
PAIRS = 4
NZ = 16


def common_model(key):
    base = jax.random.fold_in(key, 11)
    keys = jax.random.split(base, 5)
    shape = (NZ, NX, NY)
    shear = jax.random.uniform(keys[0], shape, jnp.float32, 0.5, 1.5)
    prior = jax.random.uniform(keys[1], shape, jnp.float32, 0.5, 1.5)
    levels = 1.0 + 2.0 * jnp.arange(NZ, dtype=jnp.float32) / max(NZ - 1, 1)
    noise = jax.random.normal(keys[3], (PAIRS,) + shape, jnp.float32)
    weights = jax.random.uniform(keys[2], (PAIRS, 1, 1, 1), jnp.float32, 0.5, 2.0)
    updates = levels[None, :, None, None] * (weights * (shear - prior)[None] + 0.5 * noise)
    factors = jnp.exp(jax.random.uniform(keys[4], (PAIRS,) + shape, jnp.float32, -0.6931, 0.6931))
    changes = factors * updates
    return (shear, prior, updates, changes)


def draw_shear_modulus(key, part):
    return common_model(key)[0]


def draw_prior_mean(key, part):
    return common_model(key)[1]


def draw_steps_taken(key, part):
    return common_model(key)[2]


def draw_grad_change(key, part):
    return common_model(key)[3]


def shard_levels(rng, extent, cuts, low, top_value):
    def one(dim, shards_of):
        draws = jax.random.uniform(jax.random.fold_in(jax.random.fold_in(rng, 6), dim), (shards_of,), jnp.float32, low / len(cuts), top_value / len(cuts))
        return jnp.repeat(jnp.exp(draws), extent[dim] // shards_of).reshape((-1,) + (1,) * (len(extent) - dim - 1))

    level = one(*cuts[0])
    for cut in cuts[1:]:
        level = level * one(*cut)
    return level


def gaussian(key, extent, deviation, bound, pieces=(), kind=jnp.bfloat16):
    values = jax.random.normal(key, extent, jnp.float32) * deviation
    if len(pieces) > 0:
        values = shard_levels(key, extent, pieces, -0.22, 0.18) * values
    return jnp.clip(values, min=-bound, max=bound).astype(kind)


def setup_inputs(seed: int = 0, part: int = 0) -> dict:
    arg_keys = jax.random.split(jax.random.key(seed), 11)
    part_keys = jax.random.split(jax.random.fold_in(arg_keys[10], part), 11)
    field_now = gaussian(part_keys[0], (3, NZ, NX, NY), 1.0, 6.0, ((1, 8),), jnp.float32)
    field_before = gaussian(part_keys[1], (3, NZ, NX, NY), 1.0, 6.0, ((1, 8),), jnp.float32)
    lame_lambda = jnp.clip(0.5 + 1.0 * jax.random.uniform(part_keys[2], (NZ, NX, NY), jnp.float32) ** shard_levels(part_keys[2], (NZ, NX, NY), ((0, 8),), -0.2, 0.2), 0.5, 1.5)
    shear_modulus = draw_shear_modulus(jax.random.fold_in(jax.random.fold_in(arg_keys[10], part), 71), part)
    density = jnp.clip(jnp.exp(math.log(2.0) - 0.6931472 * jax.random.uniform(part_keys[4], (NZ, NX, NY), jnp.float32) ** shard_levels(part_keys[4], (NZ, NX, NY), ((0, 8),), -0.2, 0.2)), 1.0, 2.0)
    source_field = gaussian(part_keys[5], (3, NZ, NX, NY), 1.0, 6.0, ((1, 8),), jnp.float32)
    wavelet = gaussian(part_keys[6], (STEPS,), 1.0, 4.0, (), jnp.float32)
    prior_mean = draw_prior_mean(jax.random.fold_in(jax.random.fold_in(arg_keys[10], part), 71), part)
    steps_taken = draw_steps_taken(jax.random.fold_in(jax.random.fold_in(arg_keys[10], part), 71), part)
    grad_change = draw_grad_change(jax.random.fold_in(jax.random.fold_in(arg_keys[10], part), 71), part)
    return {"field_now": field_now, "field_before": field_before, "lame_lambda": lame_lambda, "shear_modulus": shear_modulus, "density": density, "source_field": source_field, "wavelet": wavelet, "prior_mean": prior_mean, "steps_taken": steps_taken, "grad_change": grad_change}


def shifted(padded, comp, offset):
    depth = padded.shape[1] - 2
    rows = padded.shape[2] - 2
    cols = padded.shape[3] - 2
    return lax.slice(padded[comp], (1 + offset[0], 1 + offset[1], 1 + offset[2]), (1 + offset[0] + depth, 1 + offset[1] + rows, 1 + offset[2] + cols))


def vec_add(first, second):
    return (first[0] + second[0], first[1] + second[1], first[2] + second[2])


def vec_neg(first):
    return (-first[0], -first[1], -first[2])


def operate(extended, lame_first, shear):
    padded = jnp.pad(extended, ((0, 0), (0, 0), (1, 1), (1, 1)))
    units = ((1, 0, 0), (0, 1, 0), (0, 0, 1))
    centre = (0, 0, 0)
    seconds = [[shifted(padded, comp, units[axis]) + shifted(padded, comp, vec_neg(units[axis])) - 2.0 * shifted(padded, comp, centre) for axis in range(3)] for comp in range(3)]

    def mixed(comp, first, second):
        plus_first = units[first]
        plus_second = units[second]
        return 0.25 * (shifted(padded, comp, vec_add(plus_first, plus_second)) - shifted(padded, comp, vec_add(plus_first, vec_neg(plus_second))) - shifted(padded, comp, vec_add(vec_neg(plus_first), plus_second)) + shifted(padded, comp, vec_neg(vec_add(plus_first, plus_second))))

    laplace = []
    elastic = []
    for comp in range(3):
        lap_comp = seconds[comp][0] + seconds[comp][1] + seconds[comp][2]
        grad_div = seconds[comp][comp]
        for other in range(3):
            if other != comp:
                grad_div = grad_div + mixed(other, comp, other)
        laplace.append(lap_comp)
        elastic.append((lame_first + shear) * grad_div + shear * lap_comp)
    return jnp.stack(elastic), jnp.stack(laplace)


def reference(field_now, field_before, lame_lambda, shear_modulus, density, source_field, wavelet, prior_mean, steps_taken, grad_change):
    coeff = 0.04 / density
    current = field_now
    earlier = field_before
    correlation = jnp.zeros(shear_modulus.shape, jnp.float32)
    for step in range(STEPS):
        extended = jnp.pad(current, ((0, 0), (1, 1), (0, 0), (0, 0)))
        elastic, laplace = operate(extended, lame_lambda, shear_modulus)
        correlation = correlation + jnp.sum(current * laplace, axis=0)
        nxt = 2.0 * current - earlier + coeff * (elastic + wavelet[step] * source_field)
        earlier = current
        current = nxt
    gradient = (shear_modulus - prior_mean) + 0.02 * correlation
    curv = [jnp.sum(steps_taken[i] * grad_change[i]) for i in range(PAIRS)]
    query = gradient
    alphas = [None] * PAIRS
    for i in reversed(range(PAIRS)):
        alphas[i] = jnp.sum(steps_taken[i] * query) / curv[i]
        query = query - alphas[i] * grad_change[i]
    newest = grad_change[PAIRS - 1]
    result = (curv[PAIRS - 1] / jnp.sum(newest * newest)) * query
    for i in range(PAIRS):
        beta = jnp.sum(grad_change[i] * result) / curv[i]
        result = result + (alphas[i] - beta) * steps_taken[i]
    return current, gradient, -result
```

```python
import functools

import jax
import jax.numpy as jnp
from jax import lax
from jax.experimental import pallas as pl
from jax.experimental.pallas import tpu as pltpu
from jax.sharding import PartitionSpec as P

PAD = 8
CHUNK_ROWS = 16


def chunk_rows(rows):
    size = CHUNK_ROWS
    while rows % size:
        size //= 2
    return size


def tile(start):
    return pl.ds(pl.multiple_of(start, 8), 8)


def kernel(
    n,
    steps,
    pairs,
    size,
    now_hbm,
    before_hbm,
    lame_hbm,
    shear_hbm,
    density_hbm,
    source_hbm,
    wavelet,
    prior_hbm,
    taken_hbm,
    change_hbm,
    final_hbm,
    gradient_hbm,
    direction_hbm,
    even,
    odd,
    lame,
    shear,
    coeff,
    source,
    prior,
    taken,
    change,
    grad,
    direction,
    sums,
    part,
    gathered,
    load_sem,
    store_sem,
    send_sem,
    recv_sem,
    part_send,
    part_recv,
):
    me = lax.axis_index("gz")
    rows, cols = lame.shape[1], lame.shape[2]
    chunks = rows // size
    tiles = size // 8
    has_low = me > 0
    has_high = me < n - 1
    inside = pl.ds(PAD, rows)

    loads = [
        pltpu.make_async_copy(src, dst, load_sem.at[i])
        for i, (src, dst) in enumerate(
            (
                (now_hbm, even.at[:, pl.ds(1, 2), inside]),
                (lame_hbm, lame),
                (shear_hbm, shear),
                (density_hbm, coeff),
                (before_hbm, odd.at[:, pl.ds(1, 2), inside]),
                (source_hbm, source),
                (taken_hbm, taken),
                (change_hbm, change),
                (prior_hbm, prior),
            )
        )
    ]
    for load in loads:
        load.start()

    barrier = pltpu.get_barrier_semaphore()
    for k in range(1, n):
        pl.semaphore_signal(
            barrier,
            inc=1,
            device_id={"gz": lax.rem(me + k, n)},
            device_id_type=pl.DeviceIdType.MESH,
        )

    edge = jnp.zeros((even.shape[0], 4, PAD, cols), jnp.float32)
    for ref in (even, odd):
        ref[:, :, pl.ds(0, PAD)] = edge
        ref[:, :, pl.ds(PAD + rows, PAD)] = edge

    def clear(plane):
        def body(t, carry):
            for ref in (even, odd):
                for comp in range(3):
                    ref[comp, plane, tile(PAD + 8 * t)] = jnp.zeros((8, cols), jnp.float32)
            return carry

        lax.fori_loop(0, rows // 8, body, 0)

    @pl.when(me == 0)
    def _():
        clear(0)

    @pl.when(me == n - 1)
    def _():
        clear(3)

    def rdma(ref, parity, up, chunk):
        where = pl.ds(pl.multiple_of(PAD + chunk * size, 8), size)
        side = 0 if up else 1
        target = lax.rem(me + (1 if up else n - 1), n)
        return pltpu.make_async_remote_copy(
            src_ref=ref.at[:, 2 if up else 1, where],
            dst_ref=ref.at[:, 0 if up else 3, where],
            send_sem=send_sem.at[parity, side, chunk],
            recv_sem=recv_sem.at[parity, side, chunk],
            device_id={"gz": target},
            device_id_type=pl.DeviceIdType.MESH,
        )

    def send(ref, parity, chunk):
        @pl.when(has_high)
        def _():
            rdma(ref, parity, True, chunk).start()

        @pl.when(has_low)
        def _():
            rdma(ref, parity, False, chunk).start()

    def sent(ref, parity, chunk):
        @pl.when(has_high)
        def _():
            rdma(ref, parity, True, chunk).wait_send()

        @pl.when(has_low)
        def _():
            rdma(ref, parity, False, chunk).wait_send()

    def received(ref, parity, chunk):
        @pl.when(has_low)
        def _():
            rdma(ref, parity, True, chunk).wait_recv()

        @pl.when(has_high)
        def _():
            rdma(ref, parity, False, chunk).wait_recv()

    loads[0].wait()
    pl.semaphore_wait(barrier, n - 1)

    def first(chunk, carry):
        send(even, 0, chunk)
        return carry

    lax.fori_loop(0, chunks, first, 0)

    for load in loads[1:4]:
        load.wait()

    def prepare(t, carry):
        for plane in range(2):
            at = (plane, tile(8 * t))
            lame[at] = lame[at] + shear[at]
            coeff[at] = 0.04 / coeff[at]
            grad[at] = jnp.zeros((8, cols), jnp.float32)
        return carry

    lax.fori_loop(0, rows // 8, prepare, 0)
    for load in loads[4:]:
        load.wait()

    half = cols // 2
    products = [(i, pairs + j) for i in range(pairs) for j in range(pairs)]
    products += [(pairs + i, pairs + j) for i in range(pairs) for j in range(i, pairs)]
    count = len(products)
    where_of = {pair: k for k, pair in enumerate(products)}
    for i in range(2 * pairs):
        where_of[(i, 2 * pairs)] = count + i

    def fold(value):
        out = value[:, 0:128]
        for k in range(1, cols // 128):
            out = out + value[:, 128 * k : 128 * (k + 1)]
        return out

    def stored(t, totals):
        totals = list(totals)
        for plane in range(2):
            vectors = [taken[i, plane, tile(8 * t)] for i in range(pairs)]
            vectors += [change[i, plane, tile(8 * t)] for i in range(pairs)]
            for k, (a, b) in enumerate(products):
                totals[k] = totals[k] + fold(vectors[a] * vectors[b])
        return tuple(totals)

    totals = lax.fori_loop(
        0, rows // 8, stored, tuple(jnp.zeros((8, 128), jnp.float32) for _ in products)
    )
    place = lax.broadcasted_iota(jnp.int32, (1, 128), 1)

    def whole(value):
        return jnp.sum(jnp.sum(value, axis=0, keepdims=True), axis=1, keepdims=True)

    line = jnp.zeros((1, 128), jnp.float32)
    for k in range(count):
        line = jnp.where(place == k, whole(totals[k]), line)
    part[...] = line
    for i in range(2 * pairs):
        sums[i] = jnp.zeros((8, 128), jnp.float32)

    row_at = lax.broadcasted_iota(jnp.int32, (8, cols), 0)
    col_at = lax.broadcasted_iota(jnp.int32, (8, cols), 1)
    is_top, is_bottom = row_at == 0, row_at == 7
    is_left, is_right = col_at == 0, col_at == cols - 1

    def along_x(previous, value, following):
        minus = pltpu.roll(jnp.where(is_bottom, previous, value), 1, 0)
        plus = pltpu.roll(jnp.where(is_top, following, value), 7, 0)
        return minus, plus

    def along_y(value):
        minus = jnp.where(is_left, 0.0, pltpu.roll(value, 1, 1))
        plus = jnp.where(is_right, 0.0, pltpu.roll(value, cols - 1, 1))
        return minus, plus

    def delta_y(value):
        minus, plus = along_y(value)
        return plus - minus

    def update(step, current, other, t):
        amplitude = wavelet[step]

        def load(comp, plane, shift=0):
            return current[comp, plane, tile(PAD + 8 * (t + shift))]

        for plane in range(2):
            low, mid, high = plane, plane + 1, plane + 2
            at = tile(8 * t)
            here = tile(PAD + 8 * t)

            def delta_z(comp, shift=0):
                return load(comp, high, shift) - load(comp, low, shift)

            def delta_xz(comp, centre):
                minus, plus = along_x(delta_z(comp, -1), centre, delta_z(comp, 1))
                return plus - minus

            centre = [load(comp, mid) for comp in range(3)]
            diff = [delta_z(comp) for comp in range(3)]
            total = [load(comp, high) + load(comp, low) for comp in range(3)]
            xs = [along_x(load(comp, mid, -1), centre[comp], load(comp, mid, 1)) for comp in range(3)]
            ys = [along_y(centre[comp]) for comp in range(3)]
            sum_x = [minus + plus for minus, plus in xs]
            sum_y = [minus + plus for minus, plus in ys]
            dx = [plus - minus for minus, plus in xs]
            lap = [
                (total[comp] + sum_x[comp]) + (sum_y[comp] - 6.0 * centre[comp])
                for comp in range(3)
            ]
            mixed = [
                delta_xz(1, diff[1]) + delta_y(diff[2]),
                delta_xz(0, diff[0]) + delta_y(dx[2]),
                delta_y(diff[0] + dx[1]),
            ]
            own = [total[0], sum_x[1], sum_y[2]]
            both = lame[plane, at]
            mu = shear[plane, at]
            rate = coeff[plane, at]
            grad[plane, at] = grad[plane, at] + (
                centre[0] * lap[0] + centre[1] * lap[1] + centre[2] * lap[2]
            )
            for comp in range(3):
                doubled = 2.0 * centre[comp]
                elastic = both * ((own[comp] - doubled) + 0.25 * mixed[comp]) + mu * lap[comp]
                other[comp, mid, here] = (
                    doubled
                    - other[comp, mid, here]
                    + rate * (elastic + amplitude * source[comp, plane, at])
                )

    def finish(t, totals):
        totals = list(totals)
        for plane in range(2):
            at = (plane, tile(8 * t))
            value = (shear[at] - prior[at]) + 0.02 * grad[at]
            grad[at] = value
            for i in range(pairs):
                totals[i] = totals[i] + fold(taken[(i,) + at] * value)
                totals[pairs + i] = totals[pairs + i] + fold(change[(i,) + at] * value)
        return tuple(totals)

    def advance(step, current, other, parity):
        received(current, parity, 0)

        def chunk_body(chunk, carry):
            @pl.when(chunk + 1 < chunks)
            def _():
                received(current, parity, chunk + 1)

            @pl.when(step > 0)
            def _():
                sent(other, 1 - parity, chunk)

            def tile_body(t, inner):
                update(step, current, other, chunk * tiles + t)
                return inner

            lax.fori_loop(0, tiles, tile_body, 0)

            @pl.when(step < steps - 1)
            def _():
                send(other, 1 - parity, chunk)

            if parity == 1:

                @pl.when(step == steps - 1)
                def _():
                    totals = lax.fori_loop(
                        chunk * tiles,
                        chunk * tiles + tiles,
                        finish,
                        tuple(sums[i] for i in range(2 * pairs)),
                    )
                    for i in range(2 * pairs):
                        sums[i] = totals[i]

            return carry

        lax.fori_loop(0, chunks, chunk_body, 0)

    def two_steps(k, carry):
        advance(2 * k, even, odd, 0)
        advance(2 * k + 1, odd, even, 1)
        return carry

    lax.fori_loop(0, steps // 2, two_steps, 0)

    line = part[...]
    for i in range(2 * pairs):
        line = jnp.where(place == count + i, whole(sums[i]), line)
    part[...] = line

    outs = [
        pltpu.make_async_copy(grad, gradient_hbm, store_sem.at[0]),
        pltpu.make_async_copy(even.at[:, pl.ds(1, 2), inside], final_hbm, store_sem.at[1]),
        pltpu.make_async_copy(direction, direction_hbm, store_sem.at[2]),
    ]
    exchange = [
        pltpu.make_async_remote_copy(
            src_ref=part,
            dst_ref=gathered.at[k - 1],
            send_sem=part_send.at[k - 1],
            recv_sem=part_recv.at[k - 1],
            device_id={"gz": lax.rem(me + k, n)},
            device_id_type=pl.DeviceIdType.MESH,
        )
        for k in range(1, n)
    ]
    for copy in exchange:
        copy.start()
    outs[0].start()
    outs[1].start()

    def last_sent(chunk, carry):
        sent(odd, 1, chunk)
        return carry

    lax.fori_loop(0, chunks, last_sent, 0)
    for copy in exchange:
        copy.wait_recv()
    line = part[...]
    for k in range(n - 1):
        line = line + gathered[k]

    def product(a, b):
        k = where_of[(min(a, b), max(a, b))]
        return jnp.sum(jnp.where(place == k, line, 0.0), axis=1, keepdims=True)

    cache = {}

    def inner(a, b):
        key = (min(a, b), max(a, b))
        if key not in cache:
            cache[key] = product(*key)
        return cache[key]

    gradient_at = 2 * pairs
    curvature = [inner(i, pairs + i) for i in range(pairs)]
    alphas = [None] * pairs
    for i in reversed(range(pairs)):
        value = inner(i, gradient_at)
        for j in range(i + 1, pairs):
            value = value - alphas[j] * inner(i, pairs + j)
        alphas[i] = value / curvature[i]
    newest = 2 * pairs - 1
    gamma = curvature[pairs - 1] / inner(newest, newest)
    changes = [-gamma * alphas[i] for i in range(pairs)]
    steps_coef = [None] * pairs
    for i in range(pairs):
        value = gamma * inner(pairs + i, gradient_at)
        for j in range(pairs):
            value = value + changes[j] * inner(pairs + i, pairs + j)
        for j in range(i):
            value = value + steps_coef[j] * inner(j, pairs + i)
        steps_coef[i] = alphas[i] - value / curvature[i]

    def spread(value):
        return -jnp.broadcast_to(value, (8, cols))

    by_grad = spread(gamma)
    by_taken = [spread(value) for value in steps_coef]
    by_change = [spread(value) for value in changes]

    def combine(t, carry):
        for plane in range(2):
            at = (plane, tile(8 * t))
            value = by_grad * grad[at]
            for i in range(pairs):
                value = value + by_taken[i] * taken[(i,) + at]
                value = value + by_change[i] * change[(i,) + at]
            direction[at] = value
        return carry

    lax.fori_loop(0, rows // 8, combine, 0)
    outs[2].start()
    for copy in exchange:
        copy.wait_send()
    for out in outs:
        out.wait()


def on_device(
    n,
    field_now,
    field_before,
    lame_lambda,
    shear_modulus,
    density,
    source_field,
    wavelet,
    prior_mean,
    steps_taken,
    grad_change,
):
    comps, depth, rows, cols = field_now.shape
    pairs = steps_taken.shape[0]
    steps = wavelet.shape[0]
    size = chunk_rows(rows)
    chunks = rows // size
    f32 = jnp.float32
    state = pltpu.VMEM((comps, depth + 2, rows + 2 * PAD, cols), f32)
    model = pltpu.VMEM((depth, rows, cols), f32)
    stored = pltpu.VMEM((pairs, depth, rows, cols), f32)
    dma = pltpu.SemaphoreType.DMA
    anywhere = pl.BlockSpec(memory_space=pl.ANY)
    return pl.pallas_call(
        functools.partial(kernel, n, steps, pairs, size),
        out_shape=(
            jax.ShapeDtypeStruct(field_now.shape, f32),
            jax.ShapeDtypeStruct(lame_lambda.shape, f32),
            jax.ShapeDtypeStruct(lame_lambda.shape, f32),
        ),
        in_specs=[anywhere] * 6
        + [pl.BlockSpec(memory_space=pltpu.SMEM)]
        + [anywhere] * 3,
        out_specs=(anywhere, anywhere, anywhere),
        scratch_shapes=[
            state,
            state,
            model,
            model,
            model,
            pltpu.VMEM((comps, depth, rows, cols), f32),
            model,
            stored,
            stored,
            model,
            model,
            pltpu.VMEM((2 * pairs, 8, 128), f32),
            pltpu.VMEM((1, 128), f32),
            pltpu.VMEM((n - 1, 1, 128), f32),
            dma((9,)),
            dma((3,)),
            dma((2, 2, chunks)),
            dma((2, 2, chunks)),
            dma((n - 1,)),
            dma((n - 1,)),
        ],
        compiler_params=pltpu.CompilerParams(
            collective_id=0, has_side_effects=True, vmem_limit_bytes=48 * 1024 * 1024
        ),
    )(
        field_now,
        field_before,
        lame_lambda,
        shear_modulus,
        density,
        source_field,
        wavelet,
        prior_mean,
        steps_taken,
        grad_change,
    )


def solution(mesh):
    n = mesh.shape["gz"]
    fields = P("sample", "gz", None, None)
    models = P("gz", "sample", None)
    placed = (
        fields,
        fields,
        models,
        models,
        models,
        fields,
        P("sample"),
        models,
        fields,
        fields,
    )
    return jax.shard_map(
        functools.partial(on_device, n),
        mesh=mesh,
        in_specs=placed,
        out_specs=(fields, models, models),
        check_vma=False,
    )
```

```python
import functools

import jax
import jax.numpy as jnp
from jax import lax
from jax.experimental import pallas as pl
from jax.experimental.pallas import tpu as pltpu
from jax.sharding import PartitionSpec as P

PAD = 8
CHUNK_ROWS = 16


def chunk_rows(rows):
    size = CHUNK_ROWS
    while rows % size:
        size //= 2
    return size


def tile(start):
    return pl.ds(pl.multiple_of(start, 8), 8)


def kernel(
    n,
    steps,
    pairs,
    size,
    now_hbm,
    before_hbm,
    lame_hbm,
    shear_hbm,
    density_hbm,
    source_hbm,
    wavelet,
    prior_hbm,
    taken_hbm,
    change_hbm,
    final_hbm,
    grad,
    direction,
    even,
    odd,
    lame,
    shear,
    coeff,
    source,
    prior,
    taken,
    change,
    sums,
    part,
    gathered,
    load_sem,
    store_sem,
    send_sem,
    recv_sem,
    part_send,
    part_recv,
):
    me = lax.axis_index("gz")
    rows, cols = lame.shape[1], lame.shape[2]
    chunks = rows // size
    tiles = size // 8
    has_low = me > 0
    has_high = me < n - 1
    inside = pl.ds(PAD, rows)

    loads = [
        pltpu.make_async_copy(src, dst, load_sem.at[i])
        for i, (src, dst) in enumerate(
            (
                (now_hbm, even.at[:, pl.ds(1, 2), inside]),
                (lame_hbm, lame),
                (shear_hbm, shear),
                (density_hbm, coeff),
                (before_hbm, odd.at[:, pl.ds(1, 2), inside]),
                (source_hbm, source),
                (taken_hbm, taken),
                (change_hbm, change),
                (prior_hbm, prior),
            )
        )
    ]
    for load in loads:
        load.start()

    barrier = pltpu.get_barrier_semaphore()
    for k in range(1, n):
        pl.semaphore_signal(
            barrier,
            inc=1,
            device_id={"gz": lax.rem(me + k, n)},
            device_id_type=pl.DeviceIdType.MESH,
        )

    edge = jnp.zeros((even.shape[0], 4, PAD, cols), jnp.float32)
    for ref in (even, odd):
        ref[:, :, pl.ds(0, PAD)] = edge
        ref[:, :, pl.ds(PAD + rows, PAD)] = edge

    def clear(plane):
        def body(t, carry):
            for ref in (even, odd):
                for comp in range(3):
                    ref[comp, plane, tile(PAD + 8 * t)] = jnp.zeros((8, cols), jnp.float32)
            return carry

        lax.fori_loop(0, rows // 8, body, 0)

    @pl.when(me == 0)
    def _():
        clear(0)

    @pl.when(me == n - 1)
    def _():
        clear(3)

    def rdma(ref, parity, up, chunk):
        where = pl.ds(pl.multiple_of(PAD + chunk * size, 8), size)
        side = 0 if up else 1
        target = lax.rem(me + (1 if up else n - 1), n)
        return pltpu.make_async_remote_copy(
            src_ref=ref.at[:, 2 if up else 1, where],
            dst_ref=ref.at[:, 0 if up else 3, where],
            send_sem=send_sem.at[parity, side, chunk],
            recv_sem=recv_sem.at[parity, side, chunk],
            device_id={"gz": target},
            device_id_type=pl.DeviceIdType.MESH,
        )

    def send(ref, parity, chunk):
        @pl.when(has_high)
        def _():
            rdma(ref, parity, True, chunk).start()

        @pl.when(has_low)
        def _():
            rdma(ref, parity, False, chunk).start()

    def sent(ref, parity, chunk):
        @pl.when(has_high)
        def _():
            rdma(ref, parity, True, chunk).wait_send()

        @pl.when(has_low)
        def _():
            rdma(ref, parity, False, chunk).wait_send()

    def received(ref, parity, chunk):
        @pl.when(has_low)
        def _():
            rdma(ref, parity, True, chunk).wait_recv()

        @pl.when(has_high)
        def _():
            rdma(ref, parity, False, chunk).wait_recv()

    loads[0].wait()
    pl.semaphore_wait(barrier, n - 1)

    def first(chunk, carry):
        send(even, 0, chunk)
        return carry

    lax.fori_loop(0, chunks, first, 0)

    for load in loads[1:4]:
        load.wait()

    def prepare(t, carry):
        for plane in range(2):
            at = (plane, tile(8 * t))
            lame[at] = lame[at] + shear[at]
            coeff[at] = 0.04 / coeff[at]
            grad[at] = jnp.zeros((8, cols), jnp.float32)
        return carry

    lax.fori_loop(0, rows // 8, prepare, 0)
    for load in loads[4:]:
        load.wait()

    half = cols // 2
    products = [(i, pairs + j) for i in range(pairs) for j in range(pairs)]
    products += [(pairs + i, pairs + j) for i in range(pairs) for j in range(i, pairs)]
    count = len(products)
    where_of = {pair: k for k, pair in enumerate(products)}
    for i in range(2 * pairs):
        where_of[(i, 2 * pairs)] = count + i

    def fold(value):
        out = value[:, 0:128]
        for k in range(1, cols // 128):
            out = out + value[:, 128 * k : 128 * (k + 1)]
        return out

    def stored(t, totals):
        totals = list(totals)
        for plane in range(2):
            vectors = [taken[i, plane, tile(8 * t)] for i in range(pairs)]
            vectors += [change[i, plane, tile(8 * t)] for i in range(pairs)]
            for k, (a, b) in enumerate(products):
                totals[k] = totals[k] + fold(vectors[a] * vectors[b])
        return tuple(totals)

    totals = lax.fori_loop(
        0, rows // 8, stored, tuple(jnp.zeros((8, 128), jnp.float32) for _ in products)
    )
    place = lax.broadcasted_iota(jnp.int32, (1, 128), 1)

    def whole(value):
        return jnp.sum(jnp.sum(value, axis=0, keepdims=True), axis=1, keepdims=True)

    line = jnp.zeros((1, 128), jnp.float32)
    for k in range(count):
        line = jnp.where(place == k, whole(totals[k]), line)
    part[...] = line
    for i in range(2 * pairs):
        sums[i] = jnp.zeros((8, 128), jnp.float32)

    row_at = lax.broadcasted_iota(jnp.int32, (8, cols), 0)
    col_at = lax.broadcasted_iota(jnp.int32, (8, cols), 1)
    is_top, is_bottom = row_at == 0, row_at == 7
    is_left, is_right = col_at == 0, col_at == cols - 1

    def along_x(previous, value, following):
        minus = pltpu.roll(jnp.where(is_bottom, previous, value), 1, 0)
        plus = pltpu.roll(jnp.where(is_top, following, value), 7, 0)
        return minus, plus

    def along_y(value):
        minus = jnp.where(is_left, 0.0, pltpu.roll(value, 1, 1))
        plus = jnp.where(is_right, 0.0, pltpu.roll(value, cols - 1, 1))
        return minus, plus

    def delta_y(value):
        minus, plus = along_y(value)
        return plus - minus

    def update(step, current, other, t):
        amplitude = wavelet[step]

        def load(comp, plane, shift=0):
            return current[comp, plane, tile(PAD + 8 * (t + shift))]

        for plane in range(2):
            low, mid, high = plane, plane + 1, plane + 2
            at = tile(8 * t)
            here = tile(PAD + 8 * t)

            def delta_z(comp, shift=0):
                return load(comp, high, shift) - load(comp, low, shift)

            def delta_xz(comp, centre):
                minus, plus = along_x(delta_z(comp, -1), centre, delta_z(comp, 1))
                return plus - minus

            centre = [load(comp, mid) for comp in range(3)]
            diff = [delta_z(comp) for comp in range(3)]
            total = [load(comp, high) + load(comp, low) for comp in range(3)]
            xs = [along_x(load(comp, mid, -1), centre[comp], load(comp, mid, 1)) for comp in range(3)]
            ys = [along_y(centre[comp]) for comp in range(3)]
            sum_x = [minus + plus for minus, plus in xs]
            sum_y = [minus + plus for minus, plus in ys]
            dx = [plus - minus for minus, plus in xs]
            lap = [
                (total[comp] + sum_x[comp]) + (sum_y[comp] - 6.0 * centre[comp])
                for comp in range(3)
            ]
            mixed = [
                delta_xz(1, diff[1]) + delta_y(diff[2]),
                delta_xz(0, diff[0]) + delta_y(dx[2]),
                delta_y(diff[0] + dx[1]),
            ]
            own = [total[0], sum_x[1], sum_y[2]]
            both = lame[plane, at]
            mu = shear[plane, at]
            rate = coeff[plane, at]
            grad[plane, at] = grad[plane, at] + (
                centre[0] * lap[0] + centre[1] * lap[1] + centre[2] * lap[2]
            )
            for comp in range(3):
                doubled = 2.0 * centre[comp]
                elastic = both * ((own[comp] - doubled) + 0.25 * mixed[comp]) + mu * lap[comp]
                other[comp, mid, here] = (
                    doubled
                    - other[comp, mid, here]
                    + rate * (elastic + amplitude * source[comp, plane, at])
                )

    def finish(t, totals):
        totals = list(totals)
        for plane in range(2):
            at = (plane, tile(8 * t))
            value = (shear[at] - prior[at]) + 0.02 * grad[at]
            grad[at] = value
            for i in range(pairs):
                totals[i] = totals[i] + fold(taken[(i,) + at] * value)
                totals[pairs + i] = totals[pairs + i] + fold(change[(i,) + at] * value)
        return tuple(totals)

    def advance(step, current, other, parity):
        received(current, parity, 0)

        def chunk_body(chunk, carry):
            @pl.when(chunk + 1 < chunks)
            def _():
                received(current, parity, chunk + 1)

            @pl.when(step > 0)
            def _():
                sent(other, 1 - parity, chunk)

            def tile_body(t, inner):
                update(step, current, other, chunk * tiles + t)
                return inner

            lax.fori_loop(0, tiles, tile_body, 0)

            @pl.when(step < steps - 1)
            def _():
                send(other, 1 - parity, chunk)

            if parity == 1:

                @pl.when(step == steps - 1)
                def _():
                    totals = lax.fori_loop(
                        chunk * tiles,
                        chunk * tiles + tiles,
                        finish,
                        tuple(sums[i] for i in range(2 * pairs)),
                    )
                    for i in range(2 * pairs):
                        sums[i] = totals[i]

            return carry

        lax.fori_loop(0, chunks, chunk_body, 0)

    def two_steps(k, carry):
        advance(2 * k, even, odd, 0)
        advance(2 * k + 1, odd, even, 1)
        return carry

    lax.fori_loop(0, steps // 2, two_steps, 0)

    line = part[...]
    for i in range(2 * pairs):
        line = jnp.where(place == count + i, whole(sums[i]), line)
    part[...] = line

    out = pltpu.make_async_copy(even.at[:, pl.ds(1, 2), inside], final_hbm, store_sem.at[0])
    exchange = [
        pltpu.make_async_remote_copy(
            src_ref=part,
            dst_ref=gathered.at[k - 1],
            send_sem=part_send.at[k - 1],
            recv_sem=part_recv.at[k - 1],
            device_id={"gz": lax.rem(me + k, n)},
            device_id_type=pl.DeviceIdType.MESH,
        )
        for k in range(1, n)
    ]
    for copy in exchange:
        copy.start()
    out.start()

    def last_sent(chunk, carry):
        sent(odd, 1, chunk)
        return carry

    lax.fori_loop(0, chunks, last_sent, 0)
    for copy in exchange:
        copy.wait_recv()
    line = part[...]
    for k in range(n - 1):
        line = line + gathered[k]

    def product(a, b):
        k = where_of[(min(a, b), max(a, b))]
        return jnp.sum(jnp.where(place == k, line, 0.0), axis=1, keepdims=True)

    cache = {}

    def inner(a, b):
        key = (min(a, b), max(a, b))
        if key not in cache:
            cache[key] = product(*key)
        return cache[key]

    gradient_at = 2 * pairs
    curvature = [inner(i, pairs + i) for i in range(pairs)]
    alphas = [None] * pairs
    for i in reversed(range(pairs)):
        value = inner(i, gradient_at)
        for j in range(i + 1, pairs):
            value = value - alphas[j] * inner(i, pairs + j)
        alphas[i] = value / curvature[i]
    newest = 2 * pairs - 1
    gamma = curvature[pairs - 1] / inner(newest, newest)
    changes = [-gamma * alphas[i] for i in range(pairs)]
    steps_coef = [None] * pairs
    for i in range(pairs):
        value = gamma * inner(pairs + i, gradient_at)
        for j in range(pairs):
            value = value + changes[j] * inner(pairs + i, pairs + j)
        for j in range(i):
            value = value + steps_coef[j] * inner(j, pairs + i)
        steps_coef[i] = alphas[i] - value / curvature[i]

    def spread(value):
        return -jnp.broadcast_to(value, (8, cols))

    by_grad = spread(gamma)
    by_taken = [spread(value) for value in steps_coef]
    by_change = [spread(value) for value in changes]

    def combine(t, carry):
        for plane in range(2):
            at = (plane, tile(8 * t))
            value = by_grad * grad[at]
            for i in range(pairs):
                value = value + by_taken[i] * taken[(i,) + at]
                value = value + by_change[i] * change[(i,) + at]
            direction[at] = value
        return carry

    lax.fori_loop(0, rows // 8, combine, 0)
    for copy in exchange:
        copy.wait_send()
    out.wait()


def on_device(
    n,
    field_now,
    field_before,
    lame_lambda,
    shear_modulus,
    density,
    source_field,
    wavelet,
    prior_mean,
    steps_taken,
    grad_change,
):
    comps, depth, rows, cols = field_now.shape
    pairs = steps_taken.shape[0]
    steps = wavelet.shape[0]
    size = chunk_rows(rows)
    chunks = rows // size
    f32 = jnp.float32
    state = pltpu.VMEM((comps, depth + 2, rows + 2 * PAD, cols), f32)
    model = pltpu.VMEM((depth, rows, cols), f32)
    stored = pltpu.VMEM((pairs, depth, rows, cols), f32)
    dma = pltpu.SemaphoreType.DMA
    anywhere = pl.BlockSpec(memory_space=pltpu.HBM)
    free = pl.BlockSpec(memory_space=pl.ANY)
    results = pl.pallas_call(
        functools.partial(kernel, n, steps, pairs, size),
        out_shape=(
            pltpu.VMEM(field_now.shape, f32),
            pltpu.VMEM(lame_lambda.shape, f32),
            pltpu.VMEM(lame_lambda.shape, f32),
        ),
        in_specs=[anywhere] * 6
        + [pl.BlockSpec(memory_space=pltpu.SMEM)]
        + [anywhere] * 3,
        out_specs=(pl.BlockSpec(memory_space=pltpu.VMEM),) * 3,
        scratch_shapes=[
            state,
            state,
            model,
            model,
            model,
            pltpu.VMEM((comps, depth, rows, cols), f32),
            model,
            stored,
            stored,
            pltpu.VMEM((2 * pairs, 8, 128), f32),
            pltpu.VMEM((1, 128), f32),
            pltpu.VMEM((n - 1, 1, 128), f32),
            dma((9,)),
            dma((1,)),
            dma((2, 2, chunks)),
            dma((2, 2, chunks)),
            dma((n - 1,)),
            dma((n - 1,)),
        ],
        compiler_params=pltpu.CompilerParams(
            collective_id=0, has_side_effects=True, vmem_limit_bytes=65000000
        ),
    )(
        field_now,
        field_before,
        lame_lambda,
        shear_modulus,
        density,
        source_field,
        wavelet,
        prior_mean,
        steps_taken,
        grad_change,
    )
    return pl.pallas_call(
        publish,
        out_shape=tuple(jax.ShapeDtypeStruct(value.shape, f32) for value in results),
        in_specs=[free] * 3,
        out_specs=(free, free, free),
        scratch_shapes=[dma((3,))],
        compiler_params=pltpu.CompilerParams(vmem_limit_bytes=1024 * 1024),
    )(*[pltpu.with_memory_space_constraint(value, pltpu.VMEM) for value in results])


def publish(*refs):
    sem = refs[-1]
    copies = [pltpu.make_async_copy(refs[i], refs[3 + i], sem.at[i]) for i in range(3)]
    for copy in copies:
        copy.start()
    for copy in copies:
        copy.wait()


def solution(mesh):
    n = mesh.shape["gz"]
    fields = P("sample", "gz", None, None)
    models = P("gz", "sample", None)
    placed = (
        fields,
        fields,
        models,
        models,
        models,
        fields,
        P("sample"),
        models,
        fields,
        fields,
    )
    return jax.shard_map(
        functools.partial(on_device, n),
        mesh=mesh,
        in_specs=placed,
        out_specs=(fields, models, models),
        check_vma=False,
    )
```
